32 devices in a mesh: dp: 32 (over z, y, x, core).
Axes of the slice: x: 2, y: 2, z: 4, core: 2. Of those that a mesh axis runs over, the one named last changes fastest.
Arguments:
- master: float32 [65536], P('dp'), may hold values from -6 to 6
- gradients: float32 [65536], P('dp'), may hold values from -6 to 6
- first_moment: float32 [65536], P('dp'), may hold values from -4 to 4
- second_moment: float32 [65536], P('dp'), may hold values from 0.01 to 1
- segment_ids: int32 [65536], P('dp'), may hold values from 0 to 63, as said below
- decay_mask: int32 [64], replicated, may hold values 0 or 1
Outputs:
- new_master: float32 [65536], P('dp')
- new_first: float32 [65536], P('dp')
- new_second: float32 [65536], P('dp')
- scaled_step: float32 [65536], P('dp')
- model_weights: bfloat16 [65536], replicated
The draws below stay inside these ranges and needn't reach their ends.
Inputs may be any that keep to these rules, and one draw needn't show every extreme that they name: segment_ids never falls along the flat vector; each tensor 0 to 63 owns one contiguous run of 256 to 16384 elements, and one tensor has exactly 16384. `decay_mask`: each entry is 0 or 1.
All inputs are finite; a program needn't handle non-finite values.
Results may differ from the reference program's by a relative error of at most 0.0004.
Values may be sent and summed in bfloat16 or wider, within the bound.
A program may use at most 64 MiB of HBM per device.

```python
import math
import jax
import jax.numpy as jnp

P_DEV = 2048
SEG_DEV = 2
STEP = 20
PARAMS = 65536
TENSORS = 64


def draw_segment_ids(key, part):
    weight_key = jax.random.fold_in(key, 11)
    place_key = jax.random.fold_in(key, 23)
    shortest = P_DEV // (4 * SEG_DEV)
    longest = 8 * P_DEV
    shares = jax.random.randint(weight_key, (TENSORS - 1,), 1, 8).astype(jnp.int32)
    remain = PARAMS - longest - (TENSORS - 1) * shortest
    total = jnp.sum(shares)
    running = jnp.cumsum(shares)
    bounds = remain // total * running + remain % total * running // total
    extra = jnp.diff(jnp.concatenate([jnp.zeros((1,), jnp.int32), bounds.astype(jnp.int32)]))
    others = shortest + extra
    place = jax.random.randint(place_key, (), 0, TENSORS).astype(jnp.int32)
    tensor_index = jnp.arange(TENSORS, dtype=jnp.int32)
    source = jnp.clip(tensor_index - (tensor_index > place).astype(jnp.int32), 0, TENSORS - 2)
    lengths = jnp.where(tensor_index == place, longest, others[source]).astype(jnp.int32)
    finish = jnp.cumsum(lengths)
    positions = jnp.arange(PARAMS, dtype=jnp.int32)
    return jnp.searchsorted(finish, positions, side='right').astype(jnp.int32)


def set_ends(entries, own_key, low, largest):
    spot = [jax.random.randint(jax.random.fold_in(own_key, axis), (), 0, length) for axis, length in enumerate(entries.shape)]
    widest = entries.shape.index(max(entries.shape))
    next_to = spot[:widest] + [(spot[widest] + 1) % entries.shape[widest]] + spot[widest + 1:]
    return entries.at[tuple(spot)].set(low).at[tuple(next_to)].set(largest)


def levels(own_key, shape, pieces, least, high):
    def one(position, parts):
        heights = jax.random.uniform(jax.random.fold_in(jax.random.fold_in(own_key, 6), position), (parts,), jnp.float32, least / len(pieces), high / len(pieces))
        return jnp.repeat(jnp.exp(heights), shape[position] // parts).reshape((-1,) + (1,) * (len(shape) - position - 1))

    loudness = one(*pieces[0])
    for cut in pieces[1:]:
        loudness = loudness * one(*cut)
    return loudness


def normal_values(own_key, shape, scale, reach, split=(), held_as=jnp.bfloat16):
    array = jax.random.normal(own_key, shape, jnp.float32) * scale
    if len(split) > 0:
        array = levels(own_key, shape, split, -0.22, 0.18) * array
    return jnp.clip(array, min=-reach, max=reach).astype(held_as)


def setup_inputs(seed: int = 0) -> dict:
    streams_of = jax.random.split(jax.random.key(seed), 7)
    master = normal_values(streams_of[0], (PARAMS,), 1.0, 6.0, ((0, 32),), jnp.float32)
    gradients = normal_values(streams_of[1], (PARAMS,), 1.0, 6.0, ((0, 32),), jnp.float32)
    first_moment = normal_values(streams_of[2], (PARAMS,), 0.3, 4.0, ((0, 32),), jnp.float32)
    second_moment = jnp.clip(jnp.exp(math.log(1.0) - 4.6051702 * jax.random.uniform(streams_of[3], (PARAMS,), jnp.float32) ** levels(streams_of[3], (PARAMS,), ((0, 32),), -0.2, 0.2)), 0.01, 1.0)
    segment_ids = draw_segment_ids(jax.random.fold_in(streams_of[6], 71), 0)
    decay_mask = set_ends((jax.random.randint(streams_of[5], (TENSORS,), 0, 2) < 1).astype(jnp.int32), jax.random.fold_in(streams_of[5], 1), 0, 1)
    return {"master": master, "gradients": gradients, "first_moment": first_moment, "second_moment": second_moment, "segment_ids": segment_ids, "decay_mask": decay_mask}


first_decay = 0.9
second_decay = 0.999
epsilon = 1e-06
weight_decay = 0.01
learn_rate = 0.006

def adam_direction(master, gradients, first_moment, second_moment, decay):
    new_first = first_decay * first_moment + (1.0 - first_decay) * gradients
    new_second = second_decay * second_moment + (1.0 - second_decay) * gradients * gradients
    hat_first = new_first / (1.0 - first_decay ** STEP)
    hat_second = new_second / (1.0 - second_decay ** STEP)
    direction = hat_first / (jnp.sqrt(hat_second) + epsilon) + weight_decay * decay * master
    return (new_first, new_second, direction)

def trust_ratio(weight_sq, step_sq):
    weight_norm = jnp.sqrt(weight_sq)
    step_norm = jnp.sqrt(step_sq)
    usable = (weight_norm > 0.0) & (step_norm > 0.0)
    return jnp.where(usable, weight_norm / jnp.where(usable, step_norm, 1.0), 1.0)

def reference(master, gradients, first_moment, second_moment, segment_ids, decay_mask):
    decay = decay_mask.astype(jnp.float32)[segment_ids]
    new_first, new_second, direction = adam_direction(master, gradients, first_moment, second_moment, decay)
    weight_sq = jax.ops.segment_sum(master * master, segment_ids, num_segments=TENSORS)
    step_sq = jax.ops.segment_sum(direction * direction, segment_ids, num_segments=TENSORS)
    scaled_step = trust_ratio(weight_sq, step_sq)[segment_ids] * direction
    new_master = master - learn_rate * scaled_step
    return (new_master, new_first, new_second, scaled_step, new_master.astype(jnp.bfloat16))
```

```python
import functools

import jax
import jax.numpy as jnp
from jax import lax
from jax.experimental import pallas as pl
from jax.experimental.pallas import tpu as pltpu
from jax.sharding import PartitionSpec as P

STEP = 20
LANES = 128
SHORTEST_RUN = 256
LONGEST_RUN = 16384

first_decay = 0.9
second_decay = 0.999
epsilon = 1e-06
weight_decay = 0.01
learn_rate = 0.006

MESH = pl.DeviceIdType.MESH


def total_of(values):
    return jnp.sum(jnp.sum(values, axis=0, keepdims=True), axis=1, keepdims=True)


def kernel(
    n,
    radius,
    local,
    master_hbm,
    gradients_hbm,
    first_hbm,
    second_hbm,
    ids_hbm,
    mask_hbm,
    new_master_hbm,
    new_first_hbm,
    new_second_hbm,
    scaled_hbm,
    weights_hbm,
    inputs,
    ids_vmem,
    edge_ids,
    mask_smem,
    outputs,
    weights_vmem,
    to_right,
    to_left,
    received,
    load_sem,
    store_sem,
    near_send,
    near_recv,
    far_send,
    far_recv,
):
    me = lax.axis_index("dp")
    rows = master_hbm.shape[0]
    tensors = mask_hbm.shape[0]

    received[...] = jnp.zeros_like(received)
    barrier = pltpu.get_barrier_semaphore()
    for distance in range(1, n):
        pl.semaphore_signal(
            barrier, inc=1, device_id=(lax.rem(me + distance, n),), device_id_type=MESH
        )

    loads = [
        pltpu.make_async_copy(source, target, load_sem.at[position])
        for position, (source, target) in enumerate(
            [
                (ids_hbm.at[pl.ds(0, 1)], edge_ids.at[pl.ds(0, 1)]),
                (ids_hbm.at[pl.ds(rows - 1, 1)], edge_ids.at[pl.ds(1, 1)]),
                (mask_hbm, mask_smem),
                (ids_hbm, ids_vmem),
                (first_hbm, inputs.at[2]),
                (gradients_hbm, inputs.at[1]),
                (second_hbm, inputs.at[3]),
                (master_hbm, inputs.at[0]),
            ]
        )
    ]
    for load in loads:
        load.start()
    for load in loads:
        load.wait()

    first_id = edge_ids[0, 0]
    last_id = edge_ids[1, LANES - 1]
    ids = ids_vmem[...]
    is_last = ids == last_id
    inside = [ids == first_id + k for k in range(local)]
    decay = jnp.zeros(ids.shape, jnp.float32)
    for k in range(local):
        entry = mask_smem[jnp.minimum(first_id + k, tensors - 1)].astype(jnp.float32)
        decay = jnp.where(inside[k], entry, decay)

    master = inputs[0]
    gradients = inputs[1]
    new_first = first_decay * inputs[2] + (1.0 - first_decay) * gradients
    new_second = second_decay * inputs[3] + (1.0 - second_decay) * gradients * gradients
    hat_first = new_first / (1.0 - first_decay**STEP)
    hat_second = new_second / (1.0 - second_decay**STEP)
    direction = hat_first / (jnp.sqrt(hat_second) + epsilon) + weight_decay * decay * master
    weight_square = master * master
    step_square = direction * direction

    def sums(chosen):
        return (
            total_of(jnp.where(chosen, weight_square, 0.0)),
            total_of(jnp.where(chosen, step_square, 0.0)),
        )

    weight_first, step_first = sums(inside[0])
    weight_last, step_last = sums(is_last)
    lane = lax.broadcasted_iota(jnp.int32, (1, LANES), 1)

    def message(segment, weight, step):
        return jnp.where(
            lane == 0, segment.astype(jnp.float32), jnp.where(lane == 1, weight, step)
        )

    to_right[...] = message(last_id, weight_last, step_last)
    to_left[...] = message(first_id, weight_first, step_first)
    outputs[1] = new_first
    outputs[2] = new_second

    pl.semaphore_wait(barrier, n - 1)

    def near_copy(source, slot, target):
        return pltpu.make_async_remote_copy(
            src_ref=source,
            dst_ref=received.at[pl.ds(slot, 1)],
            send_sem=near_send.at[slot],
            recv_sem=near_recv.at[slot],
            device_id=(target,),
            device_id_type=MESH,
        )

    for distance in range(radius, 0, -1):

        @pl.when(me + distance < n)
        def _():
            near_copy(to_right, distance - 1, me + distance).start()

        @pl.when(me >= distance)
        def _():
            near_copy(to_left, radius + distance - 1, me - distance).start()

    stores = [
        pltpu.make_async_copy(outputs.at[1], new_first_hbm, store_sem.at[0]),
        pltpu.make_async_copy(outputs.at[2], new_second_hbm, store_sem.at[1]),
    ]
    for store in stores:
        store.start()

    middle = [sums(inside[k]) for k in range(1, local)]

    for distance in range(1, radius + 1):

        @pl.when(me >= distance)
        def _():
            near_copy(to_right, distance - 1, me - distance).wait_recv()

        @pl.when(me + distance < n)
        def _():
            near_copy(to_left, radius + distance - 1, me + distance).wait_recv()

    table = received[...]
    segment_column = table[:, 0:1]

    def gathered(segment):
        found = jnp.where(segment_column == segment.astype(jnp.float32), table, 0.0)
        found = jnp.sum(found, axis=0, keepdims=True)
        return found[:, 1:2], found[:, 2:3]

    weight_more, step_more = gathered(first_id)
    weight_sq = jnp.broadcast_to(weight_first + weight_more, ids.shape)
    step_sq = jnp.broadcast_to(step_first + step_more, ids.shape)
    for k in range(1, local):
        weight_sq = jnp.where(inside[k], middle[k - 1][0], weight_sq)
        step_sq = jnp.where(inside[k], middle[k - 1][1], step_sq)
    weight_more, step_more = gathered(last_id)
    weight_sq = jnp.where(is_last, weight_last + weight_more, weight_sq)
    step_sq = jnp.where(is_last, step_last + step_more, step_sq)

    weight_norm = jnp.sqrt(weight_sq)
    step_norm = jnp.sqrt(step_sq)
    usable = (weight_norm > 0.0) & (step_norm > 0.0)
    trust = jnp.where(usable, weight_norm / jnp.where(usable, step_norm, 1.0), 1.0)
    scaled_step = trust * direction
    new_master = master - learn_rate * scaled_step
    weights_vmem[...] = new_master.astype(jnp.bfloat16)
    outputs[3] = scaled_step
    outputs[0] = new_master

    mine = weights_hbm.at[pl.ds(pl.multiple_of(me * rows, rows), rows)]

    def far_copy(distance):
        return pltpu.make_async_remote_copy(
            src_ref=weights_vmem,
            dst_ref=mine,
            send_sem=far_send.at[distance - 1],
            recv_sem=far_recv.at[distance - 1],
            device_id=(lax.rem(me + distance, n),),
            device_id_type=MESH,
        )

    for distance in range(1, n):
        far_copy(distance).start()
    for position, (source, target) in enumerate(
        [
            (weights_vmem, mine),
            (outputs.at[3], scaled_hbm),
            (outputs.at[0], new_master_hbm),
        ]
    ):
        store = pltpu.make_async_copy(source, target, store_sem.at[2 + position])
        store.start()
        stores.append(store)

    for distance in range(1, radius + 1):

        @pl.when(me + distance < n)
        def _():
            near_copy(to_right, distance - 1, me + distance).wait_send()

        @pl.when(me >= distance)
        def _():
            near_copy(to_left, radius + distance - 1, me - distance).wait_send()

    for store in stores:
        store.wait()
    for distance in range(1, n):
        far_copy(distance).wait_send()
    for distance in range(1, n):
        far_copy(distance).wait_recv()


def solution(mesh):
    n = mesh.shape["dp"]

    def shards(master, gradients, first_moment, second_moment, segment_ids, decay_mask):
        length = master.shape[0]
        rows = length // LANES
        tensors = decay_mask.shape[0]
        radius = min(n - 1, (LONGEST_RUN - 2) // length + 1)
        local = min(tensors, (length - 2) // SHORTEST_RUN + 2)
        block = jax.ShapeDtypeStruct((rows, LANES), jnp.float32)
        flat = [
            x.reshape(rows, LANES)
            for x in (master, gradients, first_moment, second_moment, segment_ids)
        ]
        anywhere = pl.BlockSpec(memory_space=pl.ANY)
        outs = pl.pallas_call(
            functools.partial(kernel, n, radius, local),
            out_shape=(block,) * 4 + (jax.ShapeDtypeStruct((n * rows, LANES), jnp.bfloat16),),
            in_specs=[anywhere] * 6,
            out_specs=(anywhere,) * 5,
            scratch_shapes=[
                pltpu.VMEM((4, rows, LANES), jnp.float32),
                pltpu.VMEM((rows, LANES), jnp.int32),
                pltpu.SMEM((2, LANES), jnp.int32),
                pltpu.SMEM((tensors,), jnp.int32),
                pltpu.VMEM((4, rows, LANES), jnp.float32),
                pltpu.VMEM((rows, LANES), jnp.bfloat16),
                pltpu.VMEM((1, LANES), jnp.float32),
                pltpu.VMEM((1, LANES), jnp.float32),
                pltpu.VMEM((2 * radius, LANES), jnp.float32),
                pltpu.SemaphoreType.DMA((8,)),
                pltpu.SemaphoreType.DMA((5,)),
                pltpu.SemaphoreType.DMA((2 * radius,)),
                pltpu.SemaphoreType.DMA((2 * radius,)),
                pltpu.SemaphoreType.DMA((n - 1,)),
                pltpu.SemaphoreType.DMA((n - 1,)),
            ],
            compiler_params=pltpu.CompilerParams(collective_id=0, has_side_effects=True),
        )(*flat, decay_mask)
        return tuple(x.reshape(-1) for x in outs)

    in_specs = (P("dp"), P("dp"), P("dp"), P("dp"), P("dp"), P())
    out_specs = (P("dp"), P("dp"), P("dp"), P("dp"), P())
    return jax.shard_map(shards, mesh=mesh, in_specs=in_specs, out_specs=out_specs, check_vma=False)
```
